256 devices in a mesh: expert: 32 (over z_lo, y, core), tensor: 8 (over z_hi, x).
Axes of the slice: x: 4, y: 4, z: 8 (z_hi: 2, z_lo: 4; z = z_hi * 4 + z_lo), core: 2. Of those that a mesh axis runs over, the one named last changes fastest.
Arguments:
- tokens: bfloat16 [32768, 2048], P(('expert', 'tensor')), may hold values from -6 to 6
- assignment: int32 [32768], P(('expert', 'tensor')), may hold values from 0 to 31, as said below
- norm_gain: float32 [2048], replicated, may hold values from 0.25 to 1.75
- centroids: bfloat16 [32, 2048], replicated, may hold values from -0.125 to 0.125
- w_in: bfloat16 [32, 2048, 8192], P('expert', None, 'tensor'), may hold values from -0.125 to 0.125
- w_out: bfloat16 [32, 8192, 2048], P('expert', 'tensor'), may hold values from -0.0625 to 0.0625
Outputs:
- mixed: bfloat16 [32768, 2048], P(('expert', 'tensor'))
The draws below stay inside these ranges and needn't reach their ends.
Inputs may be any that keep to these rules, and one draw needn't show every extreme that they name: `assignment`: in each device's block of 128 consecutive tokens every expert is named exactly 4 times.
All inputs are finite; a program needn't handle non-finite values.
Results may differ from the reference program's by a relative error of at most 0.006.
Values may be sent and summed in bfloat16 or wider, within the bound.
No kernel may reach another device: no remote copies, remote signals or barrier semaphores. Data moves between devices by JAX's collectives and lax.ppermute only.
A program may use at most 64 MiB of HBM per device.

```python
import jax
import jax.numpy as jnp
from jax import lax

D = 2048
FF = 8192
TOK_DEV = 128
EXPERTS = 32
TOKENS = 32768
N_TENSOR = 8


def draw_assignment(key, part):
    block_keys = jax.random.split(key, TOKENS // TOK_DEV)

    def shuffled(sub_key):
        return jax.random.permutation(sub_key, TOK_DEV) % EXPERTS
    return jax.vmap(shuffled)(block_keys).reshape(TOKENS).astype(jnp.int32)


def block_scale(stream_key, shape, shards, low, largest):
    level, own = 1.0, jax.random.fold_in(stream_key, 6)
    for position, blocks in shards:
        heights = jnp.exp(jax.random.uniform(jax.random.fold_in(own, position), (blocks,), jnp.float32, low / len(shards), largest / len(shards)))
        level = level * jnp.repeat(heights, shape[position] // blocks).reshape([-1 if axis == position else 1 for axis in range(len(shape))])
    return level


def normal_values(rng, dims, spread, most, cuts=(), kind=jnp.bfloat16):
    loudness = block_scale(rng, dims, cuts, -0.22, 0.18) if cuts else 1.0
    entries = jax.random.normal(rng, dims, jnp.float32) * spread * loudness
    return jnp.minimum(jnp.maximum(entries, -most), most).astype(kind)


def setup_inputs(seed: int = 0) -> dict:
    key_of = jax.random.split(jax.random.key(seed), 7)
    tokens = normal_values(key_of[0], (TOKENS, D), 1.0, 6.0, ((0, 256),))
    assignment = draw_assignment(jax.random.fold_in(key_of[6], 71), 0)
    norm_gain = jnp.clip(1.0 + 0.15 * jax.random.normal(key_of[2], (D,), jnp.float32), 0.25, 1.75)
    centroids = normal_values(key_of[3], (EXPERTS, D), D ** -0.5, 0.125)
    w_in = normal_values(key_of[4], (EXPERTS, D, FF), D ** -0.5, 0.125, ((0, 32), (2, 8)))
    w_out = normal_values(key_of[5], (EXPERTS, FF, D), FF ** -0.5, 0.0625, ((0, 32), (1, 8)))
    return dict(tokens=tokens, assignment=assignment, norm_gain=norm_gain, centroids=centroids, w_in=w_in, w_out=w_out)


def layer_norm(values, gain):
    widened = values.astype(jnp.float32)
    average = lax.optimization_barrier(jnp.mean(widened, axis=1, keepdims=True))
    centred = widened - average
    variance = lax.optimization_barrier(jnp.mean(centred * centred, axis=1, keepdims=True))
    return centred * lax.rsqrt(variance + 1e-05) * gain

def reference(tokens, assignment, norm_gain, centroids, w_in, w_out):
    normed = layer_norm(tokens, norm_gain).astype(jnp.bfloat16)
    logits = jnp.dot(tokens, centroids.T, preferred_element_type=jnp.float32)
    column_ids = jnp.arange(EXPERTS, dtype=jnp.int32)
    picked = lax.optimization_barrier(jnp.sum(jnp.where(assignment[:, None] == column_ids[None, :], logits, 0.0), axis=1))
    gate_value = jax.nn.sigmoid(picked)
    ordering = jnp.argsort(assignment, stable=True).astype(jnp.int32)
    grouped = normed[ordering].reshape(EXPERTS, TOKENS // EXPERTS, D)
    block_width = FF // N_TENSOR

    def expert_ffn(operands):
        expert_rows, w_first, w_second = operands
        hidden = jax.nn.gelu(jnp.dot(expert_rows, w_first, preferred_element_type=jnp.float32), approximate=True).astype(jnp.bfloat16)
        blocked_hidden = hidden.reshape(hidden.shape[0], N_TENSOR, block_width).astype(jnp.float32)
        blocked_weight = w_second.reshape(N_TENSOR, block_width, D).astype(jnp.float32)
        block_sum = jnp.einsum('rbf,bfd->brd', blocked_hidden, blocked_weight).astype(jnp.bfloat16)
        return lax.optimization_barrier(jnp.sum(block_sum.astype(jnp.float32), axis=0)).astype(jnp.bfloat16)
    results = lax.map(expert_ffn, (grouped, w_in, w_out)).reshape(TOKENS, D)
    expert_out = jnp.zeros((TOKENS, D), jnp.bfloat16).at[ordering].set(results)
    mixed = tokens.astype(jnp.float32) + gate_value[:, None] * expert_out.astype(jnp.float32)
    return mixed.astype(jnp.bfloat16)
```

```python
import jax
import jax.numpy as jnp
from jax import lax
from jax.sharding import Mesh
from jax.sharding import PartitionSpec as P

EXPERT = ("zl", "y", "c")
ALL = ("zl", "y", "c", "zh", "x")


def step_x(value, by):
    size = lax.axis_size("x")
    return lax.ppermute(value, "x", [(i, (i + by) % size) for i in range(size)])


def swap_halves(value):
    return lax.ppermute(value, "zh", [(0, 1), (1, 0)])


def gathered(rows):
    half = rows.shape[0] // 2
    left = step_x(rows, 1)
    right = step_x(rows, -1)
    far_low = step_x(right[:half], -1)
    far_high = step_x(left[half:], 1)
    return jnp.concatenate(
        [rows, far_low, right[half:], far_high, left[:half], right[:half], left[half:]], axis=0
    )


def add(*terms):
    total = terms[0].astype(jnp.float32)
    for term in terms[1:]:
        total = total + term.astype(jnp.float32)
    return total.astype(jnp.bfloat16)


def reduced(partials):
    n = partials.shape[0] // 4
    half = n // 2
    keep = partials[:n]
    from_left = step_x(partials[n : 2 * n], 1)
    from_right = step_x(partials[2 * n : 3 * n], -1)
    to_right = add(partials[3 * n : 3 * n + half], from_left[:half])
    to_left = add(partials[3 * n + half :], from_right[:half])
    low = step_x(to_right, 1)
    high = step_x(to_left, -1)
    return jnp.concatenate(
        [add(keep[:half], from_right[half:], low), add(keep[half:], from_left[half:], high)], axis=0
    )


def layer_norm(values, gain):
    widened = values.astype(jnp.float32)
    average = jnp.mean(widened, axis=1, keepdims=True)
    centred = widened - average
    variance = jnp.mean(centred * centred, axis=1, keepdims=True)
    return centred * lax.rsqrt(variance + 1e-05) * gain


def ffn(rows, w_first, w_second):
    hidden = jax.nn.gelu(
        jnp.dot(rows, w_first, preferred_element_type=jnp.float32), approximate=True
    ).astype(jnp.bfloat16)
    return jnp.dot(hidden, w_second, preferred_element_type=jnp.float32).astype(jnp.bfloat16)


def exchanged(rows, num_experts):
    blocks = rows.reshape(num_experts, -1, rows.shape[1])
    return lax.all_to_all(blocks, EXPERT, split_axis=0, concat_axis=0, tiled=True).reshape(rows.shape)


def body(tokens, assignment, norm_gain, centroids, w_in, w_out):
    tok_rows = tokens.shape[0]
    num_experts = centroids.shape[0]
    per_expert = tok_rows // num_experts
    normed = layer_norm(tokens, norm_gain).astype(jnp.bfloat16)
    same_expert = assignment[:, None] == assignment[None, :]
    row_ids = lax.broadcasted_iota(jnp.int32, (tok_rows, tok_rows), 0)
    col_ids = lax.broadcasted_iota(jnp.int32, (tok_rows, tok_rows), 1)
    rank_in = jnp.sum((same_expert & (col_ids < row_ids)).astype(jnp.int32), axis=1)
    slot_of = assignment * per_expert + rank_in
    place = (slot_of[:, None] == col_ids).astype(jnp.bfloat16)
    ordered = lax.dot_general(
        place, normed, (((0,), (0,)), ((), ())), preferred_element_type=jnp.float32
    ).astype(jnp.bfloat16)
    own = exchanged(ordered, num_experts)
    other = swap_halves(own)
    w_first = w_in[0]
    w_second = w_out[0]
    own_sum = reduced(ffn(gathered(own), w_first, w_second))
    other_sum = reduced(ffn(gathered(other), w_first, w_second))
    summed = add(own_sum, swap_halves(other_sum))
    returned = exchanged(summed, num_experts)
    logits = jnp.dot(tokens, centroids.T, preferred_element_type=jnp.float32)
    column_ids = lax.broadcasted_iota(jnp.int32, (tok_rows, num_experts), 1)
    picked = jnp.sum(jnp.where(assignment[:, None] == column_ids, logits, 0.0), axis=1)
    gate_value = jax.nn.sigmoid(picked)
    expert_out = jnp.dot(place, returned, preferred_element_type=jnp.float32)
    mixed = tokens.astype(jnp.float32) + gate_value[:, None] * expert_out
    return mixed.astype(jnp.bfloat16)


def solution(mesh):
    finer = Mesh(mesh.devices.reshape(4, 4, 2, 2, 4), ALL)
    return jax.shard_map(
        body,
        mesh=finer,
        in_specs=(
            P(ALL, None),
            P(ALL),
            P(),
            P(),
            P(EXPERT, None, ("zh", "x")),
            P(EXPERT, ("zh", "x"), None),
        ),
        out_specs=P(ALL, None),
        check_vma=False,
    )
```
